32 devices in a mesh: rad: 4 (over z), ma: 8 (over y, x, core).
Axes of the slice: x: 2, y: 2, z: 4, core: 2. Of those that a mesh axis runs over, the one named last changes fastest.
Arguments:
- spectra: bfloat16 [32, 3, 2, 1024, 1024], P(('rad', 'ma')), may hold values from -0.19921875 to 0.19921875
- legendre: bfloat16 [1024, 1024, 512], P('ma', 'rad'), may hold values from -0.1875 to 0.1875
- selected: int32 [16], replicated, may hold values from 0 to 31, as said below
- m_order: int32 [1024], replicated, may hold values from 0 to 1023, each once
Outputs:
- shell_grid: float32 [16, 3, 2, 512, 3072], P(None, None, None, ('rad', 'ma'))
The draws below stay inside these ranges and needn't reach their ends.
Inputs may be any that keep to these rules, and one draw needn't show every extreme that they name: `selected`: 16 distinct radii, in no particular order. `m_order`: every wavenumber 0 to 1023 stands in exactly one slot.
All inputs are finite; a program needn't handle non-finite values.
Results may differ from the reference program's by a relative error of at most 0.012.
Values may be sent and summed in bfloat16 or wider, within the bound.
A program may use at most 192 MiB of HBM per device.

```python
import jax
import jax.numpy as jnp
from jax import lax

L = 1024
M = 1024
NPHI = 3072
FIELDS = 3
SEL = 16
R = 32
NTHH = 512
N_RAD = 4


def draw_selected(key, part):
    return jax.random.permutation(key, R)[:SEL].astype(jnp.int32)


def level_of(stream_key, extent, split, least, high):
    factor_of = 1.0
    for position, parts in split:
        draws = jax.random.uniform(jax.random.fold_in(jax.random.fold_in(stream_key, 6), position), (parts,), jnp.float32, least / len(split), high / len(split))
        factor_of = factor_of * jnp.repeat(jnp.exp(draws), extent[position] // parts).reshape((-1,) + (1,) * (len(extent) - 1 - position))
    return factor_of


def centred(rng, dims, deviation, reach, pieces=(), kind=jnp.bfloat16):
    factor_of = level_of(rng, dims, pieces, -0.22, 0.18) if pieces else 1.0
    drawn = jax.random.normal(rng, dims, jnp.float32) * deviation * factor_of
    return jnp.minimum(jnp.maximum(drawn, -reach), reach).astype(kind)


def setup_inputs(seed: int = 0) -> dict:
    keys = jax.random.split(jax.random.key(seed), 5)
    return {
        "spectra": centred(keys[0], (R, FIELDS, 2, M, L), 0.03, 0.19921875, ((0, 32),)),
        "legendre": centred(keys[1], (M, L, NTHH), L ** -0.5, 0.1875, ((0, 8), (1, 4))),
        "selected": draw_selected(jax.random.fold_in(keys[4], 71), 0),
        "m_order": jax.random.permutation(keys[3], M).astype(jnp.int32),
    }


def reference(spectra, legendre, selected, m_order):
    picked = spectra[selected]
    picked = picked[:, :, :, m_order, :]
    degree = jnp.arange(L, dtype=jnp.int32)
    tri_mask = degree[None, :] >= m_order[:, None]
    picked = jnp.where(tri_mask[None, None, None], picked, jnp.zeros((), jnp.bfloat16))
    width = SEL * FIELDS * 2
    coeffs = picked.reshape(width, M, L).transpose(1, 0, 2)
    m_sign = (1 - 2 * (m_order % 2)).astype(jnp.float32)
    part_len = L // N_RAD
    total = jnp.zeros((2, M, width, NTHH), jnp.float32)
    for part_index in range(N_RAD):
        first = part_index * part_len
        block = coeffs[:, :, first:first + part_len].astype(jnp.float32)
        ptab = legendre[:, first:first + part_len, :].astype(jnp.float32)
        even_sum = jnp.einsum('sil,slt->sit', block[:, :, 0::2], ptab[:, 0::2, :])
        odd_sum = jnp.einsum('sil,slt->sit', block[:, :, 1::2], ptab[:, 1::2, :])
        north_sum = (even_sum + odd_sum).astype(jnp.bfloat16)
        south_sum = (m_sign[:, None, None] * (even_sum - odd_sum)).astype(jnp.bfloat16)
        north_sum, south_sum = lax.optimization_barrier((north_sum, south_sum))
        total = total + jnp.stack([north_sum.astype(jnp.float32), south_sum.astype(jnp.float32)])
    latitude_sum = total.astype(jnp.bfloat16)
    arranged = latitude_sum.reshape(2, M, SEL, FIELDS, 2, NTHH).transpose(2, 3, 0, 5, 4, 1)
    arranged = arranged.reshape(SEL * FIELDS * 2 * NTHH, 2 * M)
    phase = (m_order[:, None] * jnp.arange(NPHI, dtype=jnp.int32)[None, :]) % NPHI
    angle = phase.astype(jnp.float32) * (2.0 * jnp.pi / NPHI)
    weight = jnp.where(m_order == 0, 1.0, 2.0).astype(jnp.float32)
    dft_table = jnp.concatenate([weight[:, None] * jnp.cos(angle), -weight[:, None] * jnp.sin(angle)], axis=0).astype(jnp.bfloat16)
    grid = jnp.dot(arranged.astype(jnp.float32), dft_table.astype(jnp.float32), preferred_element_type=jnp.float32)
    return grid.reshape(SEL, FIELDS, 2, NTHH, NPHI)
```

```python
import functools
import math

import jax
import jax.numpy as jnp
from jax import lax
from jax.experimental import pallas as pl
from jax.experimental.pallas import tpu as pltpu
from jax.sharding import PartitionSpec as P


NPHI = 3072


def round_up(value, step):
    return -(-value // step) * step


def arrange_kernel(caps, part_len, idx_ref, spec_ref, out_ref):
    groups = idx_ref.shape[0]
    first = 0
    for r, cap in enumerate(caps):
        depth = part_len * (r + 1)
        rows = idx_ref[:, first:first + cap, :].reshape(groups * cap, 1)
        hot = (lax.broadcasted_iota(jnp.int32, (groups * cap, depth), 1) == rows)
        hot = hot.astype(jnp.float32).astype(jnp.bfloat16)
        got = jnp.dot(
            hot,
            spec_ref[0, 0, 0, 0:depth, r * part_len:(r + 1) * part_len],
            preferred_element_type=jnp.float32,
        )
        out_ref[:, 0, 0, first:first + cap, :] = got.astype(jnp.bfloat16).reshape(groups, cap, part_len)
        first += cap


def arrange(spectra, idx, chunk, caps, part_len):
    field, c0, nc = chunk
    owned, _, _, wave, degrees = spectra.shape
    groups, rows, _ = idx.shape
    return pl.pallas_call(
        functools.partial(arrange_kernel, caps, part_len),
        grid=(owned, nc),
        in_specs=[
            pl.BlockSpec((groups, rows, 1), lambda o, c: (0, 0, 0)),
            pl.BlockSpec((1, 1, 1, wave, degrees), lambda o, c: (o, field, c0 + c, 0, 0)),
        ],
        out_specs=pl.BlockSpec((groups, 1, 1, rows, part_len), lambda o, c: (0, o, c, 0, 0)),
        out_shape=jax.ShapeDtypeStruct((groups, owned, nc, rows, part_len), jnp.bfloat16),
        cost_estimate=pl.CostEstimate(
            flops=2 * owned * nc * groups * sum(cap * part_len * part_len * (r + 1) for r, cap in enumerate(caps)),
            bytes_accessed=4 * nc * owned * wave * degrees,
            transcendentals=0,
        ),
        compiler_params=pltpu.CompilerParams(vmem_limit_bytes=48 * 2 ** 20),
        name="arrange",
    )(idx, spectra)


def pick_kernel(sizes, count, src_ref, first_ref, in_ref, *out_refs):
    for k, (size, out_ref) in enumerate(zip(sizes, out_refs)):
        first = pl.multiple_of(first_ref[k], 16)

        def body(n, carry, out_ref=out_ref, first=first, size=size):
            src = src_ref[n]
            for c in range(in_ref.shape[1]):
                out_ref[n, c] = in_ref[src, c, pl.ds(first, size), :]
            return carry

        lax.fori_loop(0, count, body, 0)


def pick(received, src, firsts, sizes, count):
    nc, part_len = received.shape[1], received.shape[3]
    return pl.pallas_call(
        functools.partial(pick_kernel, sizes, count),
        in_specs=[
            pl.BlockSpec(memory_space=pltpu.SMEM),
            pl.BlockSpec(memory_space=pltpu.SMEM),
            pl.BlockSpec(memory_space=pltpu.VMEM),
        ],
        out_specs=[pl.BlockSpec(memory_space=pltpu.VMEM)] * len(sizes),
        out_shape=[jax.ShapeDtypeStruct((count, nc, size, part_len), jnp.bfloat16) for size in sizes],
        cost_estimate=pl.CostEstimate(flops=2 ** 32, bytes_accessed=2 ** 23, transcendentals=0),
        compiler_params=pltpu.CompilerParams(vmem_limit_bytes=48 * 2 ** 20),
        name="pick",
    )(src, firsts, received)


def legendre_kernel(step_slots, bands, count, pieces, to_ref, perm_ref, wave_ref, base_ref, *refs):
    blocks, refs = refs[:pieces], refs[pieces:]
    tables, out_ref, coef = refs[:step_slots], refs[step_slots], refs[step_slots + 1]
    width, _, part_len = coef.shape
    nc = blocks[0].shape[1]
    band = out_ref.shape[3]
    step = pl.program_id(0)

    @pl.when(step == 0)
    def _():
        for d, block in enumerate(blocks):
            def body(n, carry, d=d, block=block):
                to = to_ref[d * count + n]

                @pl.when(to >= 0)
                def _():
                    for c in range(nc):
                        coef[to * nc + c, 0:block.shape[2], :] = block[n, c]

                return carry

            lax.fori_loop(0, count, body, 0)

    first = pl.multiple_of(step * step_slots, step_slots)
    values = jnp.swapaxes(coef[:, pl.ds(first, step_slots), :].astype(jnp.float32), 0, 1)
    degree = lax.broadcasted_iota(jnp.int32, (width, part_len), 1) + base_ref[0]
    for j in range(step_slots):
        wave = wave_ref[step * step_slots + j]
        north = jnp.where(degree >= wave, values[j], 0.0)
        odd = lax.rem(degree + wave, 2) == 1
        south = jnp.where(odd, -north, north)
        both = jnp.concatenate([north, south], axis=0).astype(jnp.bfloat16)
        got = jnp.dot(both, tables[j][0], preferred_element_type=jnp.float32).astype(jnp.bfloat16)
        for b in range(bands):
            out_ref[b, j] = got[:, b * band:(b + 1) * band]


def legendre_sums(received, to, radii, legendre, perm, wave, base, bands):
    slots, part_len, points = legendre.shape
    count, nc = received[0].shape[:2]
    width = radii * nc
    band = points // bands
    step_slots = 16
    table_specs = [
        pl.BlockSpec((1, part_len, points), lambda g, to, perm, wave, base, j=j: (perm[g * step_slots + j], 0, 0))
        for j in range(step_slots)
    ]
    grid_spec = pltpu.PrefetchScalarGridSpec(
        num_scalar_prefetch=4,
        grid=(slots // step_slots,),
        in_specs=[pl.BlockSpec(block.shape, lambda g, *_: (0, 0, 0, 0)) for block in received] + table_specs,
        out_specs=pl.BlockSpec((bands, step_slots, 2 * width, band), lambda g, *_: (0, g, 0, 0)),
        scratch_shapes=[pltpu.VMEM((width, slots, part_len), jnp.bfloat16)],
    )
    return pl.pallas_call(
        functools.partial(legendre_kernel, step_slots, bands, count, len(received)),
        grid_spec=grid_spec,
        out_shape=jax.ShapeDtypeStruct((bands, slots, 2 * width, band), jnp.bfloat16),
        cost_estimate=pl.CostEstimate(
            flops=4 * slots * width * part_len * points,
            bytes_accessed=2 * legendre.size,
            transcendentals=0,
        ),
        compiler_params=pltpu.CompilerParams(vmem_limit_bytes=48 * 2 ** 20),
        name="legendre_sums",
    )(to, perm, wave, base, *received, *([legendre] * step_slots))


def dft_kernel(lanes, weight_ref, far_cos, far_sin, near_cos, near_sin, out_ref):
    near_c, near_s = near_cos[...], near_sin[...]
    weight = weight_ref[...]
    for k in range(far_cos.shape[1]):
        fc = weight * far_cos[:, k:k + 1]
        fs = weight * far_sin[:, k:k + 1]
        at = slice(k * lanes, (k + 1) * lanes)
        out_ref[0, :, at] = (fc * near_c - fs * near_s).astype(jnp.bfloat16)
        out_ref[1, :, at] = (-(fs * near_c + fc * near_s)).astype(jnp.bfloat16)


def dft_of(waves):
    lanes = 128
    count = waves.shape[0]
    unit = 2.0 * jnp.pi / NPHI
    far = ((waves[:, None] * (lanes * jnp.arange(NPHI // lanes, dtype=jnp.int32))[None, :]) % NPHI).astype(jnp.float32) * unit
    near = ((waves[:, None] * jnp.arange(lanes, dtype=jnp.int32)[None, :]) % NPHI).astype(jnp.float32) * unit
    weight = jnp.where(waves == 0, 1.0, 2.0).astype(jnp.float32)[:, None]
    block = count // 8
    wide = NPHI // lanes
    return pl.pallas_call(
        functools.partial(dft_kernel, lanes),
        grid=(8,),
        in_specs=[pl.BlockSpec((block, 1), lambda g: (g, 0))]
        + [pl.BlockSpec((block, wide), lambda g: (g, 0))] * 2
        + [pl.BlockSpec((block, lanes), lambda g: (g, 0))] * 2,
        out_specs=pl.BlockSpec((2, block, NPHI), lambda g: (0, g, 0)),
        out_shape=jax.ShapeDtypeStruct((2, count, NPHI), jnp.bfloat16),
        cost_estimate=pl.CostEstimate(flops=2 ** 33, bytes_accessed=2 ** 24, transcendentals=0),
        name="dft_table",
    )(weight, jnp.cos(far), jnp.sin(far), jnp.cos(near), jnp.sin(near)).reshape(2 * count, NPHI)


def grid_kernel(rows, pieces, *refs):
    blocks, table_ref, (out_ref, mark_ref, lhs) = refs[:pieces], refs[pieces], refs[-3:]
    radii, _, hemis = out_ref.shape[:3]

    @pl.when(pl.program_id(0) == 0)
    def _():
        at = 0
        for block in blocks:
            if len(block.shape) == 2:
                lhs[:, at:at + block.shape[1]] = block[...]
                at += block.shape[1]
                continue
            groups, slots = block.shape[0], block.shape[5]
            for c in range(block.shape[3]):
                for a in range(groups):
                    lhs[:, at:at + slots] = block[a, :, :, c].reshape(lhs.shape[0], slots)
                    at += slots
        mark_ref[...] = jnp.zeros_like(mark_ref)

    got = jnp.dot(lhs[...], table_ref[...], preferred_element_type=jnp.float32)
    for h in range(hemis):
        for i in range(radii):
            first = (h * radii + i) * rows
            out_ref[i, 0, h] = got[first:first + rows, :]


def write_grid(pieces, table, field, radii, fields, hemis, rows, previous):
    depth = table.shape[0]
    block = 512
    height = radii * hemis * rows
    if rows % 16 or pieces[0].shape[5] % 128:
        pieces = [p.transpose(1, 2, 4, 3, 0, 5).reshape(height, -1) for p in pieces]
    in_specs = [pl.BlockSpec(p.shape, lambda g, n=p.ndim: (0,) * n) for p in pieces]
    in_specs.append(pl.BlockSpec((depth, block), lambda g: (0, g)))
    operands = [*pieces, table]
    aliases = {}
    if previous is not None:
        in_specs.append(pl.BlockSpec(memory_space=pl.ANY))
        operands.append(previous)
        aliases = {len(pieces) + 1: 0}
    return pl.pallas_call(
        functools.partial(grid_kernel, rows, len(pieces)),
        grid=(NPHI // block,),
        in_specs=in_specs,
        out_specs=[
            pl.BlockSpec((radii, 1, hemis, rows, block), lambda g: (0, field, 0, 0, g)),
            pl.BlockSpec((8, 128), lambda g: (0, 0)),
        ],
        out_shape=[
            jax.ShapeDtypeStruct((radii, fields, hemis, rows, NPHI), jnp.float32),
            jax.ShapeDtypeStruct((8, 128), jnp.float32),
        ],
        input_output_aliases=aliases,
        scratch_shapes=[pltpu.VMEM((height, depth), jnp.bfloat16)],
        cost_estimate=pl.CostEstimate(
            flops=2 * height * depth * NPHI, bytes_accessed=4 * height * NPHI, transcendentals=0
        ),
        compiler_params=pltpu.CompilerParams(vmem_limit_bytes=48 * 2 ** 20),
        name="write_grid",
    )(*operands)


def plan(spectra, legendre, tables, caps, count, chunks):
    waves, perm, own_waves, group_of, place_of, src = tables
    n_rad = lax.axis_size("rad")
    n_ma = lax.axis_size("ma")
    rad = lax.axis_index("rad")
    slots, part_len, points = legendre.shape
    band = points // n_rad
    rows_out = band // n_ma
    owned, fields = spectra.shape[:2]
    radii = group_of.shape[0]
    firsts = [sum(caps[:r]) for r in range(n_rad)]
    rows = sum(caps)
    idx = jnp.concatenate([waves[:, :cap] for cap in caps], axis=1)[:, :, None]
    steps = list(range(-(n_rad - 1), n_rad))
    sizes = [caps[n_rad - 1 + min(d, 0)] for d in steps]
    first_of = jnp.array(firsts, jnp.int32)[jnp.clip(rad + jnp.array(steps, jnp.int32), 0, n_rad - 1)]
    spot = (rad - group_of + n_rad - 1) * count + place_of
    order = jnp.arange(radii, dtype=jnp.int32)
    to = jnp.max(
        jnp.where(spot[None, :] == jnp.arange(len(steps) * count, dtype=jnp.int32)[:, None], order[None, :], -1),
        axis=1,
    )
    base = (rad * part_len).reshape(1).astype(jnp.int32)

    def band_of(sums, index, size):
        got = lax.dynamic_index_in_dim(sums, jnp.clip(index, 0, n_rad - 1), 0, keepdims=False)
        return got[:size]

    def wide_sum(*terms):
        return sum(t.astype(jnp.float32) for t in terms).astype(jnp.bfloat16)

    table = dft_of(waves.reshape(-1))
    coefs = []
    for chunk in chunks:
        sent = arrange(spectra, idx, chunk, caps, part_len)
        got = lax.all_to_all(sent, "ma", split_axis=0, concat_axis=0, tiled=True)
        got = got.reshape(n_ma * owned, chunk[2], rows, part_len)
        blocks = pick(got, src, first_of, sizes, count)
        received = []
        for d, block in zip(steps, blocks):
            pairs = [(z, z + d) for z in range(n_rad) if 0 <= z + d < n_rad]
            if d != 0:
                block = lax.ppermute(block, "rad", pairs)
            received.append(block)
        coefs.append(received)
    grid = None
    waiting = []
    for number, chunk in enumerate(chunks):
        field, _, nc = chunk
        sums = legendre_sums(coefs[number], to, radii, legendre, perm, own_waves, base, n_rad)
        up = down = None
        for k in range(1, n_rad):
            cap = caps[k - 1]
            up_own = band_of(sums, rad + n_rad - k, cap)
            down_own = band_of(sums, rad - n_rad + k, slots)
            if up is not None:
                up = jnp.pad(up, ((0, cap - up.shape[0]), (0, 0), (0, 0)))
                up_own = wide_sum(up_own, up)
                down_own = wide_sum(down_own, down)
            up = lax.ppermute(up_own, "rad", [(z, z + 1) for z in range(k)])
            down = lax.ppermute(down_own, "rad", [(z, z - 1) for z in range(n_rad - k, n_rad)])
        up = jnp.pad(up, ((0, slots - up.shape[0]), (0, 0), (0, 0)))
        total = wide_sum(band_of(sums, rad, slots), up, down)
        total = total.reshape(slots, 2 * radii * nc, n_ma, rows_out).transpose(2, 1, 3, 0)
        got = lax.all_to_all(total, "ma", split_axis=0, concat_axis=0, tiled=True)
        waiting.append(got.reshape(n_ma, 2, radii, nc, rows_out, slots))
        if number + 1 == len(chunks) or chunks[number + 1][0] != field:
            grid = write_grid(waiting, table, field, radii, fields, 2, rows_out, grid)[0]
            waiting = []
    return grid


def local(spectra, legendre, selected, m_order):
    n_rad = lax.axis_size("rad")
    n_ma = lax.axis_size("ma")
    slots, part_len, _ = legendre.shape
    owned = spectra.shape[0]
    group_size = n_ma * owned
    radii = selected.shape[0]
    ma = lax.axis_index("ma")
    grouped = m_order.reshape(n_ma, slots)
    rank = jnp.sum((grouped[:, None, :] < grouped[:, :, None]).astype(jnp.int32), axis=2)
    places = jnp.arange(slots, dtype=jnp.int32)
    at = rank[:, None, :] == places[None, :, None]
    waves = jnp.sum(jnp.where(at, grouped[:, None, :], 0), axis=2)
    perms = jnp.sum(jnp.where(at, places[None, None, :], 0), axis=2)
    perm = lax.dynamic_index_in_dim(perms, ma, 0, keepdims=False)
    own_waves = lax.dynamic_index_in_dim(waves, ma, 0, keepdims=False)
    group_of = selected // group_size
    order = jnp.arange(radii, dtype=jnp.int32)
    before = (group_of[None, :] == group_of[:, None]) & (order[None, :] < order[:, None])
    place_of = jnp.sum(before.astype(jnp.int32), axis=1)
    rad = lax.axis_index("rad")

    def tables(count):
        mine = (group_of[None, :] == rad) & (place_of[None, :] == jnp.arange(count, dtype=jnp.int32)[:, None])
        src = jnp.sum(jnp.where(mine, (selected % group_size)[None, :], 0), axis=1)
        return waves, perm, own_waves, group_of, place_of, src

    full_caps = (slots,) * n_rad
    full_count = min(radii, group_size)
    caps, fits = [], jnp.array(True)
    for r in range(n_rad):
        share = (r + 1) / n_rad
        deviation = math.sqrt(slots * share * (1 - share))
        cap = min(slots, round_up(int(slots * share + 3.0 * deviation), 16))
        caps.append(cap)
        fits = fits & jnp.all(jnp.sum((grouped < part_len * (r + 1)).astype(jnp.int32), axis=1) <= cap)
    share = 1 / n_rad
    deviation = math.sqrt(radii * share * (1 - share))
    count = min(full_count, int(radii * share + 1.2 * deviation))
    fits = fits & (jnp.max(place_of) < count)

    fields, parts = spectra.shape[1:3]
    whole = [(f, 0, parts) for f in range(fields)]
    halves = [(f, c, 1) for f in (0, fields - 1) for c in range(parts)]
    chunks = halves[:parts] + whole[1:-1] + halves[parts:]

    def narrow(spectra, legendre):
        return plan(spectra, legendre, tables(count), tuple(caps), count, chunks)

    def full(spectra, legendre):
        return plan(spectra, legendre, tables(full_count), full_caps, full_count, whole)

    return lax.cond(fits, narrow, full, spectra, legendre)


def solution(mesh):
    return jax.shard_map(
        local,
        mesh=mesh,
        in_specs=(P(("rad", "ma"), None, None, None, None), P("ma", "rad", None), P(), P()),
        out_specs=P(None, None, None, ("rad", "ma"), None),
        check_vma=False,
    )
```
